8 devices in a mesh: rep: 1 (over z), data: 2 (over y), stage: 4 (over x, core).
Axes of the slice: x: 2, y: 2, z: 1, core: 2. Of those that a mesh axis runs over, the one named last changes fastest.
Arguments:
- embeds: bfloat16 [8, 2, 384, 1536], P(('rep', 'data'))
- targets: bfloat16 [8, 2, 384, 1536], P(('rep', 'data'))
- w_qkv: bfloat16 [4, 3, 16, 96, 1536], P(('rep', 'stage'))
- w_out: bfloat16 [4, 16, 96, 1536], P(('rep', 'stage'))
- w_up: bfloat16 [4, 1536, 6144], P(('rep', 'stage'))
- w_down: bfloat16 [4, 6144, 1536], P(('rep', 'stage'))
Outputs:
- output 1: float32 [1], P('rep')
- output 2: float32 [4, 3, 16, 96, 1536], P(('rep', 'stage'))
- output 3: float32 [4, 16, 96, 1536], P(('rep', 'stage'))
- output 4: float32 [4, 1536, 6144], P(('rep', 'stage'))
- output 5: float32 [4, 6144, 1536], P(('rep', 'stage'))
- output 6: bfloat16 [8, 2, 384, 1536], P(('rep', 'data'))
All inputs are finite; a program needn't handle non-finite values.
Results may differ from the reference program's by a relative error of at most 0.0170999.
Values are sent between devices in bfloat16 or wider.
A program may use at most 1 GiB of HBM per device.

```python
import jax
import jax.numpy as jnp
from jax import lax

DATA_REPS = 2
N_STAGES = 4
N_MICRO = 4
MICRO_BATCH = 2
SEQ_LEN = 384
D_MODEL = 1536
N_HEADS = 16
HEAD_DIM = D_MODEL // N_HEADS
FFN_DIM = 4 * D_MODEL
TOTAL_MICRO = DATA_REPS * N_MICRO
NORM_EPS = 1e-6


def setup_inputs(seed: int = 0, part: int = 0) -> dict:
    part_key = jax.random.fold_in(jax.random.key(seed), part)
    keys = jax.random.split(part_key, 6)
    act_shape = (TOTAL_MICRO, MICRO_BATCH, SEQ_LEN, D_MODEL)
    model_scale = D_MODEL ** -0.5
    ffn_scale = FFN_DIM ** -0.5
    embeds = jax.random.normal(keys[0], act_shape, jnp.float32).astype(jnp.bfloat16)
    targets = jax.random.normal(keys[1], act_shape, jnp.float32).astype(jnp.bfloat16)
    w_qkv = (jax.random.normal(keys[2], (N_STAGES, 3, N_HEADS, HEAD_DIM, D_MODEL), jnp.float32) * model_scale).astype(jnp.bfloat16)
    w_out = (jax.random.normal(keys[3], (N_STAGES, N_HEADS, HEAD_DIM, D_MODEL), jnp.float32) * model_scale).astype(jnp.bfloat16)
    w_up = (jax.random.normal(keys[4], (N_STAGES, D_MODEL, FFN_DIM), jnp.float32) * model_scale).astype(jnp.bfloat16)
    w_down = (jax.random.normal(keys[5], (N_STAGES, FFN_DIM, D_MODEL), jnp.float32) * ffn_scale).astype(jnp.bfloat16)
    return {'embeds': embeds, 'targets': targets, 'w_qkv': w_qkv, 'w_out': w_out, 'w_up': w_up, 'w_down': w_down}


def bf16_cast(vals):
    return vals.astype(jnp.bfloat16).astype(jnp.float32)


def rms_norm(vals):
    return vals * lax.rsqrt(jnp.mean(vals * vals, axis=-1, keepdims=True) + NORM_EPS)


def layer_apply(act_in, w_qkv, w_out, w_up, w_down):
    normed1 = bf16_cast(rms_norm(act_in))
    qkv_proj = bf16_cast(jnp.einsum('bsd,thkd->tbhsk', normed1, w_qkv))
    scale = HEAD_DIM ** -0.5
    scores = jnp.einsum('bhqk,bhsk->bhqs', qkv_proj[0], qkv_proj[1]) * scale
    positions = jnp.arange(SEQ_LEN)
    causal = positions[:, None] >= positions[None, :]
    attn_probs = bf16_cast(jax.nn.softmax(jnp.where(causal, scores, -1e30), axis=-1))
    context = bf16_cast(jnp.einsum('bhqs,bhsk->bhqk', attn_probs, qkv_proj[2]))
    hidden = bf16_cast(act_in + jnp.einsum('bhqk,hkd->bqd', context, w_out))
    pre_act = jnp.einsum('bsd,df->bsf', bf16_cast(rms_norm(hidden)), w_up)
    upper = bf16_cast(jax.nn.gelu(pre_act, approximate=True))
    return bf16_cast(hidden + jnp.einsum('bsf,fd->bsd', upper, w_down))


def reference(embeds, targets, w_qkv, w_out, w_up, w_down):
    weights = tuple(w.astype(jnp.float32) for w in (w_qkv, w_out, w_up, w_down))
    grad_scale = 1.0 / TOTAL_MICRO
    loss_norm = 1.0 / (TOTAL_MICRO * MICRO_BATCH * SEQ_LEN * D_MODEL)

    def forward_layer(act_in, layer_w):
        return layer_apply(act_in, *layer_w), act_in

    def backward_layer(grad_out, layer_pack):
        act_in, layer_w = layer_pack
        vjp_pull = jax.vjp(layer_apply, act_in, *layer_w)[1]
        cotangents = vjp_pull(grad_out)
        return bf16_cast(cotangents[0]), cotangents[1:]

    def micro_step(carry, micro_pair):
        grad_sums, loss_sum = carry
        act_out, stash = lax.scan(forward_layer, micro_pair[0].astype(jnp.float32), weights)
        error_mb = act_out - micro_pair[1].astype(jnp.float32)
        loss_sum = loss_sum + 0.5 * jnp.sum(error_mb * error_mb) * loss_norm
        grad_seed = bf16_cast(error_mb * grad_scale)
        grad_in, layer_grads = lax.scan(backward_layer, grad_seed, (stash, weights), reverse=True)
        grad_sums = tuple(total + piece for total, piece in zip(grad_sums, layer_grads))
        return (grad_sums, loss_sum), grad_in.astype(jnp.bfloat16)

    init_carry = (tuple(jnp.zeros_like(w) for w in weights), jnp.zeros((), jnp.float32))
    (grad_sums, loss_sum), d_embeds = lax.scan(micro_step, init_carry, (embeds, targets))
    return (loss_sum.reshape(1), grad_sums[0], grad_sums[1], grad_sums[2], grad_sums[3], d_embeds)
```

```python
import functools

import jax
import jax.numpy as jnp
from jax import lax
from jax.experimental import pallas as pl
from jax.experimental.pallas import tpu as pltpu
from jax.sharding import PartitionSpec as P


NORM_EPS = 1e-6
ROWS = 128


def rms_norm(vals):
    return vals * lax.rsqrt(jnp.mean(vals * vals, axis=-1, keepdims=True) + NORM_EPS)


def gelu_tanh(vals):
    return jax.nn.gelu(vals, approximate=True)


def dot_nn(lhs, rhs):
    return lax.dot_general(lhs, rhs, (((1,), (0,)), ((), ())), preferred_element_type=jnp.float32)


def dot_nt(lhs, rhs):
    return lax.dot_general(lhs, rhs, (((1,), (1,)), ((), ())), preferred_element_type=jnp.float32)


def dot_tn(lhs, rhs):
    return lax.dot_general(lhs, rhs, (((0,), (0,)), ((), ())), preferred_element_type=jnp.float32)


def empty_arrays(*specs):
    def kernel(*refs):
        del refs

    return pl.pallas_call(
        kernel,
        out_shape=[jax.ShapeDtypeStruct(shape, dtype) for shape, dtype in specs],
        out_specs=[pl.BlockSpec(memory_space=pl.ANY)] * len(specs),
        name='empty',
    )()


def row_probs(query, keys, row0, scale):
    scores = dot_nt(query, keys) * scale
    row_id = row0 + lax.broadcasted_iota(jnp.int32, scores.shape, 0)
    col_id = lax.broadcasted_iota(jnp.int32, scores.shape, 1)
    scores = jnp.where(row_id >= col_id, scores, -1e30)
    weights = jnp.exp(scores - jnp.max(scores, axis=-1, keepdims=True))
    return weights * (1.0 / jnp.sum(weights, axis=-1, keepdims=True))


def attn_fwd_kernel(head_dim, slot_ref, q_ref, k_ref, v_ref, old_ref, out_ref):
    del slot_ref, old_ref
    seq_len, lanes = q_ref.shape[1:]
    scale = head_dim ** -0.5
    for row0 in range(0, seq_len, ROWS):
        n_cols = row0 + ROWS
        pieces = []
        for lane0 in range(0, lanes, head_dim):
            head = slice(lane0, lane0 + head_dim)
            probs = row_probs(q_ref[0, row0:n_cols, head], k_ref[0, :n_cols, head], row0, scale)
            pieces.append(dot_nn(probs.astype(jnp.bfloat16), v_ref[0, :n_cols, head]).astype(jnp.bfloat16))
        out_ref[0, row0:n_cols, :] = jnp.concatenate(pieces, axis=1)


def attn_bwd_kernel(head_dim, n_groups, slot_ref, q_ref, k_ref, v_ref, dctx_ref, old_ref, out_ref):
    del slot_ref, old_ref
    seq_len, lanes = q_ref.shape[1:]
    scale = head_dim ** -0.5
    n_rows = seq_len // ROWS
    dq_rows = [[] for _ in range(n_rows)]
    dk_rows = [[] for _ in range(n_rows)]
    dv_rows = [[] for _ in range(n_rows)]
    for lane0 in range(0, lanes, head_dim):
        head = slice(lane0, lane0 + head_dim)
        dk_sum = [None] * n_rows
        dv_sum = [None] * n_rows
        for row_blk in range(n_rows):
            row0 = row_blk * ROWS
            n_cols = row0 + ROWS
            query = q_ref[0, row0:n_cols, head]
            keys = k_ref[0, :n_cols, head]
            dctx = dctx_ref[row0:n_cols, head]
            probs = row_probs(query, keys, row0, scale)
            d_probs = dot_nt(dctx, v_ref[0, :n_cols, head])
            delta = jnp.sum(d_probs * probs, axis=-1, keepdims=True)
            d_scores = (probs * (d_probs - delta) * scale).astype(jnp.bfloat16)
            dq_rows[row_blk].append(dot_nn(d_scores, keys).astype(jnp.bfloat16))
            dk_part = dot_tn(d_scores, query)
            dv_part = dot_tn(probs.astype(jnp.bfloat16), dctx)
            for col_blk in range(row_blk + 1):
                cols = slice(col_blk * ROWS, (col_blk + 1) * ROWS)
                if dk_sum[col_blk] is None:
                    dk_sum[col_blk] = dk_part[cols]
                    dv_sum[col_blk] = dv_part[cols]
                else:
                    dk_sum[col_blk] = dk_sum[col_blk] + dk_part[cols]
                    dv_sum[col_blk] = dv_sum[col_blk] + dv_part[cols]
        for row_blk in range(n_rows):
            dk_rows[row_blk].append(dk_sum[row_blk].astype(jnp.bfloat16))
            dv_rows[row_blk].append(dv_sum[row_blk].astype(jnp.bfloat16))
    group = pl.program_id(1)
    for kind, rows in enumerate((dq_rows, dk_rows, dv_rows)):
        lane = pl.multiple_of((kind * n_groups + group) * lanes, 128)
        for row_blk in range(n_rows):
            out_ref[0, row_blk * ROWS:(row_blk + 1) * ROWS, pl.ds(lane, lanes)] = jnp.concatenate(rows[row_blk], axis=1)


def attention_calls(n_slots, micro_b, seq_len, width, n_heads):
    head_dim = width // n_heads
    group_heads = next(g for g in range(1, n_heads + 1) if n_heads % g == 0 and (g * head_dim) % 128 == 0)
    lanes = group_heads * head_dim
    n_groups = n_heads // group_heads
    rows = micro_b * seq_len
    flops = micro_b * n_heads * seq_len * seq_len * head_dim * 4

    def qkv_spec(kind):
        return pl.BlockSpec((1, seq_len, lanes), lambda b, g, slot: (slot[0], b, kind * n_groups + g))

    def fwd(slot, qkv_st, ctx_st):
        return pl.pallas_call(
            functools.partial(attn_fwd_kernel, head_dim),
            out_shape=jax.ShapeDtypeStruct((n_slots, rows, width), jnp.bfloat16),
            grid_spec=pltpu.PrefetchScalarGridSpec(
                num_scalar_prefetch=1,
                grid=(micro_b, n_groups),
                in_specs=[qkv_spec(0), qkv_spec(1), qkv_spec(2), pl.BlockSpec(memory_space=pl.ANY)],
                out_specs=pl.BlockSpec((1, seq_len, lanes), lambda b, g, slot: (slot[0], b, g)),
            ),
            input_output_aliases={4: 0},
            cost_estimate=pl.CostEstimate(flops=flops * 6, bytes_accessed=rows * width * 8, transcendentals=0),
            compiler_params=pltpu.CompilerParams(vmem_limit_bytes=32 * 1024 * 1024),
            name='attn_fwd',
        )(slot.reshape(1), qkv_st, qkv_st, qkv_st, ctx_st)

    def bwd(slot, qkv_st, dctx, dqkv_st):
        return pl.pallas_call(
            functools.partial(attn_bwd_kernel, head_dim, n_groups),
            out_shape=jax.ShapeDtypeStruct((n_slots, rows, 3 * width), jnp.bfloat16),
            grid_spec=pltpu.PrefetchScalarGridSpec(
                num_scalar_prefetch=1,
                grid=(micro_b, n_groups),
                in_specs=[qkv_spec(0), qkv_spec(1), qkv_spec(2), pl.BlockSpec((seq_len, lanes), lambda b, g, slot: (b, g)), pl.BlockSpec(memory_space=pl.ANY)],
                out_specs=pl.BlockSpec((1, seq_len, 3 * width), lambda b, g, slot: (slot[0], b, 0)),
            ),
            input_output_aliases={5: 0},
            cost_estimate=pl.CostEstimate(flops=flops * 12, bytes_accessed=rows * width * 14, transcendentals=0),
            compiler_params=pltpu.CompilerParams(vmem_limit_bytes=40 * 1024 * 1024),
            name='attn_bwd',
        )(slot.reshape(1), qkv_st, qkv_st, qkv_st, dctx, dqkv_st)

    return fwd, bwd


def put(stack, value, slot):
    return lax.dynamic_update_index_in_dim(stack, value, slot, 0)


def get(stack, slot):
    return lax.dynamic_index_in_dim(stack, slot, 0, keepdims=False)


def solution(mesh):
    n_stages = mesh.shape['stage']
    n_data = mesh.shape['data']
    act_spec = P(('rep', 'data'))
    weight_spec = P(('rep', 'stage'))
    fast_fwd = [(src, src + 1) for src in range(0, n_stages - 1, 2)]
    slow_fwd = [(src, src + 1) for src in range(1, n_stages - 1, 2)]
    chain_fwd = [(src, src + 1) for src in range(n_stages - 1)]
    fast_bwd = [(dst, src) for src, dst in fast_fwd]
    slow_bwd = [(dst, src) for src, dst in slow_fwd]
    last_delay = (n_stages - 1) + (n_stages - 1) // 2
    swap_pairs = [
        (d * n_stages + s, ((d + 1) % n_data) * n_stages + s) for d in range(n_data) for s in (0, n_stages - 1)
    ]

    def per_device(embeds, targets, w_qkv, w_out, w_up, w_down):
        n_own, micro_b, seq_len, width = embeds.shape
        n_heads = w_qkv.shape[2]
        hidden = w_up.shape[2]
        n_micro = n_own * n_data
        rows = micro_b * seq_len
        w_qkv = w_qkv[0].reshape(3 * width, width)
        w_out = w_out[0].reshape(width, width)
        w_up = w_up[0]
        w_down = w_down[0]
        attn_fwd, attn_bwd = attention_calls(n_micro, micro_b, seq_len, width, n_heads)
        stage_idx = lax.axis_index('stage')
        data_idx = lax.axis_index('data')
        is_first = stage_idx == 0
        is_last = stage_idx == n_stages - 1
        in_by_slow = stage_idx % 2 == 0
        delay = stage_idx + stage_idx // 2
        grad_scale = 1.0 / n_micro
        loss_norm = 1.0 / (n_micro * rows * width)
        n_ticks = n_micro + last_delay
        bf16 = jnp.bfloat16

        def slot_of(turn):
            return lax.rem(turn + data_idx * n_own, n_micro)

        own = jnp.where(is_last, targets, embeds).reshape(n_own, rows, width)
        (ext, a_st, n1_st, qkv_st, ctx_st, h_st, n2_st, pre_st, u_st, g_st, dpre_st, dh_st, dqkv_st, dx_st) = empty_arrays(
            ((n_micro, rows, width), bf16),
            ((n_micro, rows, width), bf16),
            ((n_micro, rows, width), bf16),
            ((n_micro, rows, 3 * width), bf16),
            ((n_micro, rows, width), bf16),
            ((n_micro, rows, width), bf16),
            ((n_micro, rows, width), bf16),
            ((n_micro, rows, hidden), jnp.float32),
            ((n_micro, rows, hidden), bf16),
            ((n_micro, rows, width), bf16),
            ((n_micro, rows, hidden), bf16),
            ((n_micro, rows, width), bf16),
            ((n_micro, rows, 3 * width), bf16),
            ((n_own + 1, rows, width), bf16),
        )
        ext = lax.dynamic_update_slice(ext, own, (0, 0, 0))
        micro_zeros = jnp.zeros((rows, width), bf16)

        def fwd_tick(tick, carry):
            cur_in, prev_out, ext, a_st, n1_st, qkv_st, ctx_st, h_st, n2_st, pre_st, u_st, g_st, losses = carry
            swap_idx = jnp.minimum(tick, n_own - 1)
            swapped = lax.ppermute(get(ext, swap_idx), ('data', 'stage'), swap_pairs)
            slow_in = lax.ppermute(prev_out, 'stage', slow_fwd)
            turn = jnp.clip(tick - delay, 0, n_micro - 1)
            slot = slot_of(turn)
            outside = lax.optimization_barrier(get(ext, turn))
            act_in = jnp.where(is_first, outside, cur_in)
            a_st = put(a_st, act_in, slot)
            act32 = act_in.astype(jnp.float32)
            normed1 = rms_norm(act32).astype(bf16)
            n1_st = put(n1_st, normed1, slot)
            qkv_st = put(qkv_st, dot_nt(normed1, w_qkv).astype(bf16), slot)
            ctx_st = attn_fwd(slot, qkv_st, ctx_st)
            hidden16 = (act32 + dot_nn(get(ctx_st, slot), w_out)).astype(bf16)
            h_st = put(h_st, hidden16, slot)
            hidden32 = hidden16.astype(jnp.float32)
            normed2 = rms_norm(hidden32).astype(bf16)
            n2_st = put(n2_st, normed2, slot)
            pre_act = dot_nn(normed2, w_up)
            pre_st = put(pre_st, pre_act, slot)
            u_st = lax.optimization_barrier(put(u_st, gelu_tanh(pre_act).astype(bf16), slot))
            act_out = (hidden32 + dot_nn(get(u_st, slot), w_down)).astype(bf16)
            error = act_out.astype(jnp.float32) - outside.astype(jnp.float32)
            losses = put(losses, 0.5 * jnp.sum(error * error) * loss_norm, slot)
            g_st = put(g_st, (error * grad_scale).astype(bf16), slot)
            fast_in = lax.ppermute(act_out, 'stage', fast_fwd)
            hold = tick - delay >= n_micro - 1
            cur_in = jnp.where(hold, cur_in, jnp.where(in_by_slow, slow_in, fast_in))
            swapped = lax.optimization_barrier((swapped, act_out))[0]
            ext = put(ext, swapped, n_own + swap_idx)
            return cur_in, act_out, ext, a_st, n1_st, qkv_st, ctx_st, h_st, n2_st, pre_st, u_st, g_st, losses

        carry = (micro_zeros, micro_zeros, ext, a_st, n1_st, qkv_st, ctx_st, h_st, n2_st, pre_st, u_st, g_st, jnp.zeros((n_micro,), jnp.float32))
        carry = lax.fori_loop(0, n_ticks, fwd_tick, carry)
        _, _, _, a_st, n1_st, qkv_st, ctx_st, h_st, n2_st, pre_st, u_st, g_st, losses = carry

        def bwd_tick(tick, carry):
            cur_in, prev_out, chain, g_st, dpre_st, dh_st, dqkv_st, dx_st = carry
            chained = lax.ppermute(chain, 'stage', chain_fwd)
            slow_in = lax.ppermute(prev_out, 'stage', slow_bwd)
            from_last = tick - (last_delay - delay)
            slot = slot_of(jnp.clip(from_last, 0, n_micro - 1))
            grad_out = jnp.where(is_last, get(g_st, slot), cur_in)
            g_st = put(g_st, grad_out, slot)
            d_upper = dot_nt(grad_out, w_down)
            d_pre = jax.vjp(gelu_tanh, get(pre_st, slot))[1](d_upper)[0].astype(bf16)
            dpre_st = put(dpre_st, d_pre, slot)
            d_normed2 = dot_nt(d_pre, w_up)
            hidden32 = get(h_st, slot).astype(jnp.float32)
            d_hidden = grad_out.astype(jnp.float32) + jax.vjp(rms_norm, hidden32)[1](d_normed2)[0]
            d_hidden16 = d_hidden.astype(bf16)
            dh_st = put(dh_st, d_hidden16, slot)
            d_context = dot_nt(d_hidden16, w_out).astype(bf16)
            dqkv_st = attn_bwd(slot, qkv_st, d_context, dqkv_st)
            d_normed1 = dot_nn(get(dqkv_st, slot), w_qkv)
            act32 = get(a_st, slot).astype(jnp.float32)
            grad_in = (d_hidden + jax.vjp(rms_norm, act32)[1](d_normed1)[0]).astype(bf16)
            fast_in = lax.ppermute(grad_in, 'stage', fast_bwd)
            hold = from_last >= n_micro - 1
            cur_in = jnp.where(hold, cur_in, jnp.where(in_by_slow, fast_in, slow_in))
            chain = jnp.where(is_first, grad_in, chained)
            own_idx = tick - last_delay - stage_idx
            dx_st = put(dx_st, chain, jnp.where((own_idx >= 0) & (own_idx < n_own), own_idx, n_own))
            return cur_in, grad_in, chain, g_st, dpre_st, dh_st, dqkv_st, dx_st

        carry = (micro_zeros, micro_zeros, micro_zeros, g_st, dpre_st, dh_st, dqkv_st, dx_st)
        carry = lax.fori_loop(0, n_ticks, bwd_tick, carry)
        _, _, _, g_st, dpre_st, dh_st, dqkv_st, dx_st = carry

        def weight_grad(lhs_st, rhs_st):
            return lax.optimization_barrier(dot_tn(lhs_st.reshape(n_micro * rows, -1), rhs_st.reshape(n_micro * rows, -1)))

        d_qkv = weight_grad(dqkv_st, n1_st).reshape(1, 3, n_heads, width // n_heads, width)
        d_out = weight_grad(ctx_st, dh_st).reshape(1, n_heads, width // n_heads, width)
        d_up = weight_grad(n2_st, dpre_st)[None]
        d_down = weight_grad(u_st, g_st)[None]
        loss = lax.psum(jnp.where(is_last, jnp.sum(losses), 0.0), 'stage').reshape(1)
        d_embeds = dx_st[:n_own].reshape(n_own, micro_b, seq_len, width)
        return loss, d_qkv, d_out, d_up, d_down, d_embeds

    return jax.shard_map(per_device, mesh=mesh, in_specs=(act_spec, act_spec, weight_spec, weight_spec, weight_spec, weight_spec), out_specs=(P('rep'), weight_spec, weight_spec, weight_spec, weight_spec, act_spec), check_vma=False)
```

```python
import functools

import jax
import jax.numpy as jnp
from jax import lax
from jax.experimental import pallas as pl
from jax.experimental.pallas import tpu as pltpu
from jax.sharding import PartitionSpec as P


NORM_EPS = 1e-6
ROWS = 128
VMEM_BYTES = 48 * 1024 * 1024
UP_ROWS = 256
UP_COLS = 768


def rms_norm(vals):
    return vals * lax.rsqrt(jnp.mean(vals * vals, axis=-1, keepdims=True) + NORM_EPS)


def gelu_tanh(vals):
    return jax.nn.gelu(vals, approximate=True)


def dot_nn(lhs, rhs):
    return lax.dot_general(lhs, rhs, (((1,), (0,)), ((), ())), preferred_element_type=jnp.float32)


def dot_nt(lhs, rhs):
    return lax.dot_general(lhs, rhs, (((1,), (1,)), ((), ())), preferred_element_type=jnp.float32)


def dot_tn(lhs, rhs):
    return lax.dot_general(lhs, rhs, (((0,), (0,)), ((), ())), preferred_element_type=jnp.float32)


def empty_arrays(*specs):
    def kernel(*refs):
        del refs

    return pl.pallas_call(
        kernel,
        out_shape=[jax.ShapeDtypeStruct(shape, dtype) for shape, dtype in specs],
        out_specs=[pl.BlockSpec(memory_space=pl.ANY)] * len(specs),
        name='empty',
    )()


def head_spans(lanes, head_dim):
    spans = []
    for lane0 in range(0, lanes, head_dim):
        low = lane0 // 128 * 128
        high = -(-(lane0 + head_dim) // 128) * 128
        spans.append((low, high, lane0 - low, lane0 - low + head_dim))
    return spans


def keep_head(vals, first, last):
    lane = lax.broadcasted_iota(jnp.int32, vals.shape, 1)
    return jnp.where((lane >= first) & (lane < last), vals, jnp.zeros_like(vals))


def merge_heads(pieces, spans, lanes):
    blocks = []
    for low in range(0, lanes, 128):
        block = None
        for piece, (span_low, span_high, first, _) in zip(pieces, spans):
            if span_low <= low < span_high:
                part = piece[:, low - span_low:low - span_low + 128]
                if block is None:
                    block = part
                else:
                    lane = lax.broadcasted_iota(jnp.int32, part.shape, 1)
                    block = jnp.where(lane >= first + span_low - low, part, block)
        blocks.append(block)
    return jnp.concatenate(blocks, axis=1)


def row_probs(query, keys, scale):
    scores = dot_nt(query, keys)
    n_rows, n_cols = scores.shape
    row_id = lax.broadcasted_iota(jnp.int32, (n_rows, n_rows), 0)
    col_id = lax.broadcasted_iota(jnp.int32, (n_rows, n_rows), 1)
    diag = jnp.where(row_id >= col_id, scores[:, n_cols - n_rows:], -1e30)
    scores = diag if n_cols == n_rows else jnp.concatenate([scores[:, :n_cols - n_rows], diag], axis=1)
    weights = jnp.exp((scores - jnp.max(scores, axis=-1, keepdims=True)) * scale)
    return weights * (1.0 / jnp.sum(weights, axis=-1, keepdims=True))


def attn_fwd_kernel(head_dim, slot_ref, q_ref, k_ref, v_ref, old_ref, out_ref):
    del slot_ref, old_ref
    seq_len, lanes = q_ref.shape[1:]
    scale = head_dim ** -0.5
    spans = head_spans(lanes, head_dim)
    for row0 in range(0, seq_len, ROWS):
        n_cols = row0 + ROWS
        pieces = []
        for low, high, first, last in spans:
            query = keep_head(q_ref[0, row0:n_cols, low:high], first, last)
            probs = row_probs(query, k_ref[0, :n_cols, low:high], scale)
            pieces.append(dot_nn(probs.astype(jnp.bfloat16), v_ref[0, :n_cols, low:high]))
        out_ref[0, row0:n_cols, :] = merge_heads(pieces, spans, lanes).astype(jnp.bfloat16)


def attn_bwd_kernel(head_dim, n_groups, slot_ref, q_ref, k_ref, v_ref, dctx_ref, old_ref, out_ref):
    del slot_ref, old_ref
    seq_len, lanes = q_ref.shape[1:]
    scale = head_dim ** -0.5
    spans = head_spans(lanes, head_dim)
    n_rows = seq_len // ROWS
    dq_all = []
    dk_all = []
    dv_all = []
    for low, high, first, last in spans:
        dq_rows = []
        probs_rows = []
        scores_rows = []
        for row_blk in range(n_rows):
            row0 = row_blk * ROWS
            n_cols = row0 + ROWS
            query = keep_head(q_ref[0, row0:n_cols, low:high], first, last)
            dctx = keep_head(dctx_ref[row0:n_cols, low:high], first, last)
            keys = k_ref[0, :n_cols, low:high]
            probs = row_probs(query, keys, scale)
            d_probs = dot_nt(dctx, v_ref[0, :n_cols, low:high])
            delta = jnp.sum(d_probs * probs, axis=-1, keepdims=True)
            d_scores = (probs * (d_probs - delta) * scale).astype(jnp.bfloat16)
            dq_rows.append(dot_nn(d_scores, keys))
            probs_rows.append(probs.astype(jnp.bfloat16))
            scores_rows.append(d_scores)
        dk_cols = []
        dv_cols = []
        for col_blk in range(n_rows):
            cols = slice(col_blk * ROWS, (col_blk + 1) * ROWS)
            below = jnp.concatenate([scores_rows[r][:, cols] for r in range(col_blk, n_rows)], axis=0)
            dk_cols.append(dot_tn(below, q_ref[0, col_blk * ROWS:, low:high]))
            below = jnp.concatenate([probs_rows[r][:, cols] for r in range(col_blk, n_rows)], axis=0)
            dv_cols.append(dot_tn(below, dctx_ref[col_blk * ROWS:, low:high]))
        dq_all.append(dq_rows)
        dk_all.append(dk_cols)
        dv_all.append(dv_cols)
    group = pl.program_id(1)
    for kind, heads in enumerate((dq_all, dk_all, dv_all)):
        lane = pl.multiple_of((kind * n_groups + group) * lanes, 128)
        for row_blk in range(n_rows):
            merged = merge_heads([rows[row_blk] for rows in heads], spans, lanes).astype(jnp.bfloat16)
            out_ref[0, row_blk * ROWS:(row_blk + 1) * ROWS, pl.ds(lane, lanes)] = merged


def attention_calls(n_slots, micro_b, seq_len, width, n_heads):
    head_dim = width // n_heads
    group_heads = next(g for g in range(1, n_heads + 1) if n_heads % g == 0 and (g * head_dim) % 128 == 0)
    lanes = group_heads * head_dim
    n_groups = n_heads // group_heads
    rows = micro_b * seq_len
    flops = micro_b * n_heads * seq_len * seq_len * head_dim * 4

    def qkv_spec(kind):
        return pl.BlockSpec((1, seq_len, lanes), lambda b, g, slot: (slot[0], b, kind * n_groups + g))

    def fwd(slot, qkv_st, ctx_st):
        return pl.pallas_call(
            functools.partial(attn_fwd_kernel, head_dim),
            out_shape=jax.ShapeDtypeStruct((n_slots, rows, width), jnp.bfloat16),
            grid_spec=pltpu.PrefetchScalarGridSpec(
                num_scalar_prefetch=1,
                grid=(micro_b, n_groups),
                in_specs=[qkv_spec(0), qkv_spec(1), qkv_spec(2), pl.BlockSpec(memory_space=pl.ANY)],
                out_specs=pl.BlockSpec((1, seq_len, lanes), lambda b, g, slot: (slot[0], b, g)),
            ),
            input_output_aliases={4: 0},
            cost_estimate=pl.CostEstimate(flops=flops * 6, bytes_accessed=rows * width * 8, transcendentals=0),
            compiler_params=pltpu.CompilerParams(vmem_limit_bytes=VMEM_BYTES),
            name='attn_fwd',
        )(slot.reshape(1), qkv_st, qkv_st, qkv_st, ctx_st)

    def bwd(slot, qkv_st, dctx, dqkv_st):
        return pl.pallas_call(
            functools.partial(attn_bwd_kernel, head_dim, n_groups),
            out_shape=jax.ShapeDtypeStruct((n_slots, rows, 3 * width), jnp.bfloat16),
            grid_spec=pltpu.PrefetchScalarGridSpec(
                num_scalar_prefetch=1,
                grid=(micro_b, n_groups),
                in_specs=[qkv_spec(0), qkv_spec(1), qkv_spec(2), pl.BlockSpec((seq_len, lanes), lambda b, g, slot: (b, g)), pl.BlockSpec(memory_space=pl.ANY)],
                out_specs=pl.BlockSpec((1, seq_len, 3 * width), lambda b, g, slot: (slot[0], b, 0)),
            ),
            input_output_aliases={5: 0},
            cost_estimate=pl.CostEstimate(flops=flops * 12, bytes_accessed=rows * width * 14, transcendentals=0),
            compiler_params=pltpu.CompilerParams(vmem_limit_bytes=VMEM_BYTES),
            name='attn_bwd',
        )(slot.reshape(1), qkv_st, qkv_st, qkv_st, dctx, dqkv_st)

    return fwd, bwd


def up_kernel(slot_ref, n2_ref, w_ref, old_pre_ref, old_u_ref, pre_ref, u_ref):
    del slot_ref, old_pre_ref, old_u_ref
    for row0 in range(0, n2_ref.shape[1], UP_ROWS):
        rows = slice(row0, row0 + UP_ROWS)
        pre_act = dot_nn(n2_ref[0, rows, :], w_ref[...])
        pre_ref[0, rows, :] = pre_act
        u_ref[0, rows, :] = gelu_tanh(pre_act).astype(jnp.bfloat16)


def d_pre_kernel(slot_ref, g_ref, w_ref, pre_ref, old_ref, out_ref):
    del slot_ref, old_ref
    for row0 in range(0, g_ref.shape[1], UP_ROWS):
        rows = slice(row0, row0 + UP_ROWS)
        d_upper = dot_nt(g_ref[0, rows, :], w_ref[...])
        out_ref[0, rows, :] = jax.vjp(gelu_tanh, pre_ref[0, rows, :])[1](d_upper)[0].astype(jnp.bfloat16)


def hidden_calls(n_slots, rows, width, hidden):
    whole = pl.BlockSpec((1, rows, width), lambda j, slot: (slot[0], 0, 0))
    piece = pl.BlockSpec((1, rows, UP_COLS), lambda j, slot: (slot[0], 0, j))
    anywhere = pl.BlockSpec(memory_space=pl.ANY)
    params = pltpu.CompilerParams(vmem_limit_bytes=VMEM_BYTES)
    cost = pl.CostEstimate(flops=2 * rows * width * hidden, bytes_accessed=hidden * (2 * width + 6 * rows), transcendentals=0)
    stack16 = jax.ShapeDtypeStruct((n_slots, rows, hidden), jnp.bfloat16)
    stack32 = jax.ShapeDtypeStruct((n_slots, rows, hidden), jnp.float32)

    def up(slot, n2_st, w_up, pre_st, u_st):
        return pl.pallas_call(
            up_kernel,
            out_shape=(stack32, stack16),
            grid_spec=pltpu.PrefetchScalarGridSpec(
                num_scalar_prefetch=1,
                grid=(hidden // UP_COLS,),
                in_specs=[whole, pl.BlockSpec((width, UP_COLS), lambda j, slot: (0, j)), anywhere, anywhere],
                out_specs=(piece, piece),
            ),
            input_output_aliases={3: 0, 4: 1},
            cost_estimate=cost,
            compiler_params=params,
            name='up',
        )(slot.reshape(1), n2_st, w_up, pre_st, u_st)

    def d_pre(slot, g_st, w_down, pre_st, dpre_st):
        return pl.pallas_call(
            d_pre_kernel,
            out_shape=stack16,
            grid_spec=pltpu.PrefetchScalarGridSpec(
                num_scalar_prefetch=1,
                grid=(hidden // UP_COLS,),
                in_specs=[whole, pl.BlockSpec((UP_COLS, width), lambda j, slot: (j, 0)), piece, anywhere],
                out_specs=piece,
            ),
            input_output_aliases={4: 0},
            cost_estimate=cost,
            compiler_params=params,
            name='d_pre',
        )(slot.reshape(1), g_st, w_down, pre_st, dpre_st)

    return up, d_pre


def put(stack, value, slot):
    return lax.dynamic_update_index_in_dim(stack, value, slot, 0)


def get(stack, slot):
    return lax.dynamic_index_in_dim(stack, slot, 0, keepdims=False)


def solution(mesh):
    n_stages = mesh.shape['stage']
    n_data = mesh.shape['data']
    act_spec = P(('rep', 'data'))
    weight_spec = P(('rep', 'stage'))
    fast_fwd = [(src, src + 1) for src in range(0, n_stages - 1, 2)]
    slow_fwd = [(src, src + 1) for src in range(1, n_stages - 1, 2)]
    chain_fwd = [(src, src + 1) for src in range(n_stages - 1)]
    fast_bwd = [(dst, src) for src, dst in fast_fwd]
    slow_bwd = [(dst, src) for src, dst in slow_fwd]
    last_delay = (n_stages - 1) + (n_stages - 1) // 2
    swap_pairs = [
        (d * n_stages + s, ((d + 1) % n_data) * n_stages + s) for d in range(n_data) for s in (0, n_stages - 1)
    ]

    def per_device(embeds, targets, w_qkv, w_out, w_up, w_down):
        n_own, micro_b, seq_len, width = embeds.shape
        n_heads = w_qkv.shape[2]
        hidden = w_up.shape[2]
        n_micro = n_own * n_data
        rows = micro_b * seq_len
        w_qkv = w_qkv[0].reshape(3 * width, width)
        w_out = w_out[0].reshape(width, width)
        w_up = w_up[0]
        w_down = w_down[0]
        attn_fwd, attn_bwd = attention_calls(n_micro, micro_b, seq_len, width, n_heads)
        up, d_pre = hidden_calls(n_micro, rows, width, hidden)
        stage_idx = lax.axis_index('stage')
        data_idx = lax.axis_index('data')
        is_first = stage_idx == 0
        is_last = stage_idx == n_stages - 1
        in_by_slow = stage_idx % 2 == 0
        delay = stage_idx + stage_idx // 2
        grad_scale = 1.0 / n_micro
        loss_norm = 1.0 / (n_micro * rows * width)
        n_ticks = n_micro + last_delay
        bf16 = jnp.bfloat16

        def slot_of(turn):
            return lax.rem(turn + data_idx * n_own, n_micro)

        own = jnp.where(is_last, targets, embeds).reshape(n_own, rows, width)
        (ext, a_st, n1_st, qkv_st, ctx_st, h_st, n2_st, pre_st, u_st, g_st, dpre_st, dh_st, dqkv_st, dx_st) = empty_arrays(
            ((n_micro, rows, width), bf16),
            ((n_micro, rows, width), bf16),
            ((n_micro, rows, width), bf16),
            ((n_micro, rows, 3 * width), bf16),
            ((n_micro, rows, width), bf16),
            ((n_micro, rows, width), bf16),
            ((n_micro, rows, width), bf16),
            ((n_micro, rows, hidden), jnp.float32),
            ((n_micro, rows, hidden), bf16),
            ((n_micro, rows, width), bf16),
            ((n_micro, rows, hidden), bf16),
            ((n_micro, rows, width), bf16),
            ((n_micro, rows, 3 * width), bf16),
            ((n_own + 1, rows, width), bf16),
        )
        ext = lax.dynamic_update_slice(ext, own, (0, 0, 0))
        micro_zeros = jnp.zeros((rows, width), bf16)

        def fwd_tick(tick, carry):
            cur_in, prev_out, ext, a_st, n1_st, qkv_st, ctx_st, h_st, n2_st, pre_st, u_st, g_st, losses = carry
            swap_idx = jnp.minimum(tick, n_own - 1)
            swapped = lax.ppermute(get(ext, swap_idx), ('data', 'stage'), swap_pairs)
            slow_in = lax.ppermute(prev_out, 'stage', slow_fwd)
            turn = jnp.clip(tick - delay, 0, n_micro - 1)
            slot = slot_of(turn)
            outside = lax.optimization_barrier(get(ext, turn))
            act_in = jnp.where(is_first, outside, cur_in)
            a_st = put(a_st, act_in, slot)
            act32 = act_in.astype(jnp.float32)
            normed1 = rms_norm(act32).astype(bf16)
            n1_st = put(n1_st, normed1, slot)
            qkv_st = put(qkv_st, dot_nt(normed1, w_qkv).astype(bf16), slot)
            ctx_st = attn_fwd(slot, qkv_st, ctx_st)
            hidden16 = (act32 + dot_nn(get(ctx_st, slot), w_out)).astype(bf16)
            h_st = put(h_st, hidden16, slot)
            hidden32 = hidden16.astype(jnp.float32)
            normed2 = rms_norm(hidden32).astype(bf16)
            n2_st = put(n2_st, normed2, slot)
            pre_st, u_st = up(slot, n2_st, w_up, pre_st, u_st)
            act_out = (hidden32 + dot_nn(get(u_st, slot), w_down)).astype(bf16)
            error = act_out.astype(jnp.float32) - outside.astype(jnp.float32)
            losses = put(losses, 0.5 * jnp.sum(error * error) * loss_norm, slot)
            g_st = put(g_st, (error * grad_scale).astype(bf16), slot)
            fast_in = lax.ppermute(act_out, 'stage', fast_fwd)
            hold = tick - delay >= n_micro - 1
            cur_in = jnp.where(hold, cur_in, jnp.where(in_by_slow, slow_in, fast_in))
            swapped = lax.optimization_barrier((swapped, act_out))[0]
            ext = put(ext, swapped, n_own + swap_idx)
            return cur_in, act_out, ext, a_st, n1_st, qkv_st, ctx_st, h_st, n2_st, pre_st, u_st, g_st, losses

        carry = (micro_zeros, micro_zeros, ext, a_st, n1_st, qkv_st, ctx_st, h_st, n2_st, pre_st, u_st, g_st, jnp.zeros((n_micro,), jnp.float32))
        carry = lax.fori_loop(0, n_ticks, fwd_tick, carry)
        _, _, _, a_st, n1_st, qkv_st, ctx_st, h_st, n2_st, pre_st, u_st, g_st, losses = carry

        def bwd_tick(tick, carry):
            cur_in, prev_out, chain, g_st, dpre_st, dh_st, dqkv_st, dx_st = carry
            chained = lax.ppermute(chain, 'stage', chain_fwd)
            slow_in = lax.ppermute(prev_out, 'stage', slow_bwd)
            from_last = tick - (last_delay - delay)
            slot = slot_of(jnp.clip(from_last, 0, n_micro - 1))
            grad_out = jnp.where(is_last, get(g_st, slot), cur_in)
            g_st = put(g_st, grad_out, slot)
            dpre_st = d_pre(slot, g_st, w_down, pre_st, dpre_st)
            d_normed2 = dot_nt(get(dpre_st, slot), w_up)
            hidden32 = get(h_st, slot).astype(jnp.float32)
            d_hidden = grad_out.astype(jnp.float32) + jax.vjp(rms_norm, hidden32)[1](d_normed2)[0]
            d_hidden16 = d_hidden.astype(bf16)
            dh_st = put(dh_st, d_hidden16, slot)
            d_context = dot_nt(d_hidden16, w_out).astype(bf16)
            dqkv_st = attn_bwd(slot, qkv_st, d_context, dqkv_st)
            d_normed1 = dot_nn(get(dqkv_st, slot), w_qkv)
            act32 = get(a_st, slot).astype(jnp.float32)
            grad_in = (d_hidden + jax.vjp(rms_norm, act32)[1](d_normed1)[0]).astype(bf16)
            fast_in = lax.ppermute(grad_in, 'stage', fast_bwd)
            hold = from_last >= n_micro - 1
            cur_in = jnp.where(hold, cur_in, jnp.where(in_by_slow, fast_in, slow_in))
            chain = jnp.where(is_first, grad_in, chained)
            own_idx = tick - last_delay - stage_idx
            dx_st = put(dx_st, chain, jnp.where((own_idx >= 0) & (own_idx < n_own), own_idx, n_own))
            return cur_in, grad_in, chain, g_st, dpre_st, dh_st, dqkv_st, dx_st

        carry = (micro_zeros, micro_zeros, micro_zeros, g_st, dpre_st, dh_st, dqkv_st, dx_st)
        carry = lax.fori_loop(0, n_ticks, bwd_tick, carry)
        _, _, _, g_st, dpre_st, dh_st, dqkv_st, dx_st = carry

        def weight_grad(lhs_st, rhs_st):
            return lax.optimization_barrier(dot_tn(lhs_st.reshape(n_micro * rows, -1), rhs_st.reshape(n_micro * rows, -1)))

        d_qkv = weight_grad(dqkv_st, n1_st).reshape(1, 3, n_heads, width // n_heads, width)
        d_out = weight_grad(ctx_st, dh_st).reshape(1, n_heads, width // n_heads, width)
        d_up = weight_grad(n2_st, dpre_st)[None]
        d_down = weight_grad(u_st, g_st)[None]
        loss = lax.psum(jnp.where(is_last, jnp.sum(losses), 0.0), 'stage').reshape(1)
        d_embeds = dx_st[:n_own].reshape(embeds.shape)
        return loss, d_qkv, d_out, d_up, d_down, d_embeds

    return jax.shard_map(per_device, mesh=mesh, in_specs=(act_spec, act_spec, weight_spec, weight_spec, weight_spec, weight_spec), out_specs=(P('rep'), weight_spec, weight_spec, weight_spec, weight_spec, act_spec), check_vma=False)
```
